32 devices in a mesh: rows: 32 (over z, y, x, core).
Axes of the slice: x: 2, y: 2, z: 4, core: 2. Of those that a mesh axis runs over, the one named last changes fastest.
Arguments:
- tile_values: float32 [3584, 128, 128], P('rows'), as said below
- tile_row: int32 [3584], P('rows'), may hold values from 0 to 15, as said below
- tile_slot: int32 [3584], P('rows'), may hold values from 0 to 47, as said below
- tile_count: int32 [32], P('rows'), may hold values from 48 to 112, as said below
- requests: int32 [32, 32, 1], P('rows'), may hold values from 0 to 15
- right_side: float32 [512, 4, 128], P('rows')
Outputs:
- solution: float32 [512, 4, 128], P('rows')
- hessenberg: float32 [4, 4, 3], replicated
The draws below stay inside these ranges and needn't reach their ends.
Inputs may be any that keep to these rules, and one draw needn't show every extreme that they name: `tile_row`: tile t < 16 of every device lies in block row t; it is the diagonal tile of that row. `tile_slot`: slot s < 16 is the device's own block s; slot 16 + o + q is the q-th block requested from device o; tile t < 48 of every device uses slot t. `tile_count`: some device uses all 112 slots. requests[d, o, q] is a block index among device o's 16 block rows. `tile_values`: tile t < 16 of every device holds the diagonal block of its row.
All inputs are finite; a program needn't handle non-finite values.
Results may differ from the reference program's by a relative error of at most 0.0003.
Values sent between devices are 32-bit elements; how exact they have to be, the bound alone decides.
A program may use at most 64 MiB of HBM per device.

```python
import jax
import jax.numpy as jnp
from jax import lax

BS = 128
RB = 16
NRHS = 4
REQ = 1
EXTRA = 64
ITERS = 3
BLOCKS = 512
SLOTS = 48
TILES_DEV = 112
NTILES = 3584
N_ROWS = 32


def draw_tile_values(key, part):
    position = jnp.arange(NTILES, dtype=jnp.int32)
    diagonal_tile = position % TILES_DEV < RB
    spread = 0.7 / jnp.sqrt(jnp.float32(BS * TILES_DEV / RB))
    noise_key = jax.random.fold_in(key, 11)
    scale_key = jax.random.fold_in(key, 12)
    noise = jax.random.normal(noise_key, (NTILES, BS, BS), jnp.float32)
    scales = jax.random.uniform(scale_key, (NTILES, BS), jnp.float32, 1.0, 2.0)
    boosted = jnp.where(diagonal_tile[:, None], scales, 0.0)
    identity = jnp.eye(BS, dtype=jnp.float32)
    return noise * spread + boosted[:, :, None] * identity[None, :, :]


def draw_tile_row(key, part):
    position = jnp.arange(NTILES, dtype=jnp.int32) % TILES_DEV
    chosen = jax.random.randint(jax.random.fold_in(key, 21), (NTILES,), 0, RB, dtype=jnp.int32)
    return jnp.where(position < RB, position, chosen).astype(jnp.int32)


def draw_tile_slot(key, part):
    position = jnp.arange(NTILES, dtype=jnp.int32) % TILES_DEV
    chosen = jax.random.randint(jax.random.fold_in(key, 31), (NTILES,), 0, SLOTS, dtype=jnp.int32)
    return jnp.where(position < SLOTS, position, chosen).astype(jnp.int32)


def draw_tile_count(key, part):
    devices = NTILES // TILES_DEV
    level = jax.random.randint(jax.random.fold_in(key, 41), (devices,), 0, 65, dtype=jnp.int32)
    counts = SLOTS + EXTRA * level * level // 4096
    busiest = jax.random.randint(jax.random.fold_in(key, 42), (), 0, devices, dtype=jnp.int32)
    return jnp.where(jnp.arange(devices, dtype=jnp.int32) == busiest, TILES_DEV, counts).astype(jnp.int32)


def draw_right_side(key, part):
    devices = BLOCKS // RB
    owner_of = (jnp.arange(BLOCKS, dtype=jnp.int32) // RB).astype(jnp.float32)
    ramp = 1.0 + 2.0 * owner_of / max(devices - 1, 1)
    rough = jnp.exp(jax.random.uniform(jax.random.fold_in(key, 51), (BLOCKS, NRHS, 1), jnp.float32, -0.7, 0.7))
    values = jax.random.normal(jax.random.fold_in(key, 52), (BLOCKS, NRHS, BS), jnp.float32)
    return values * rough * ramp[:, None, None]


def set_ends(result, stream_key, low, high):
    place = [jax.random.randint(jax.random.fold_in(stream_key, axis), (), 0, length) for axis, length in enumerate(result.shape)]
    longest = result.shape.index(max(result.shape))
    neighbour = place[:longest] + [(place[longest] + 1) % result.shape[longest]] + place[longest + 1:]
    return result.at[tuple(place)].set(low).at[tuple(neighbour)].set(high)


def setup_inputs(seed: int = 0) -> dict:
    key_of = jax.random.split(jax.random.key(seed), 7)
    return {
        "tile_values": draw_tile_values(jax.random.fold_in(key_of[6], 71), 0),
        "tile_row": draw_tile_row(jax.random.fold_in(key_of[6], 71), 0),
        "tile_slot": draw_tile_slot(jax.random.fold_in(key_of[6], 71), 0),
        "tile_count": draw_tile_count(jax.random.fold_in(key_of[6], 71), 0),
        "requests": set_ends(jax.random.randint(key_of[4], (N_ROWS, N_ROWS, REQ), 0, RB), jax.random.fold_in(key_of[4], 1), 0, RB - 1).astype(jnp.int32),
        "right_side": draw_right_side(jax.random.fold_in(key_of[6], 71), 0),
    }


epsilon = 1e-06
highest = lax.Precision.HIGHEST

def least_squares(hessenberg, beta_norm):
    krylov = hessenberg.shape[2]
    triangle = hessenberg
    target = jnp.zeros((hessenberg.shape[0], krylov + 1), jnp.float32).at[:, 0].set(beta_norm)
    cosines = []
    sine_list = []
    for column in range(krylov):
        column_vals = triangle[:, :, column]
        for earlier in range(column):
            first_entry = column_vals[:, earlier]
            second = column_vals[:, earlier + 1]
            column_vals = column_vals.at[:, earlier].set(cosines[earlier] * first_entry + sine_list[earlier] * second)
            column_vals = column_vals.at[:, earlier + 1].set(cosines[earlier] * second - sine_list[earlier] * first_entry)
        first_entry = column_vals[:, column]
        second = column_vals[:, column + 1]
        radius = jnp.sqrt(first_entry * first_entry + second * second)
        cosine = first_entry / radius
        sine_term = second / radius
        cosines.append(cosine)
        sine_list.append(sine_term)
        column_vals = column_vals.at[:, column].set(radius).at[:, column + 1].set(0.0)
        triangle = triangle.at[:, :, column].set(column_vals)
        leading = target[:, column]
        target = target.at[:, column].set(cosine * leading).at[:, column + 1].set(-sine_term * leading)
    weights = jnp.zeros((hessenberg.shape[0], krylov), jnp.float32)
    for column in reversed(range(krylov)):
        partial_sum = target[:, column] - lax.optimization_barrier(jnp.sum(triangle[:, column, column + 1:krylov] * weights[:, column + 1:], axis=1))
        weights = weights.at[:, column].set(partial_sum / triangle[:, column, column])
    return weights

def reference(tile_values, tile_row, tile_slot, tile_count, requests, right_side):
    tile_total = tile_slot.shape[0]
    position = jnp.arange(tile_total, dtype=jnp.int32)
    device = (position // TILES_DEV).astype(jnp.int32)
    shifted = jnp.maximum(tile_slot - RB, 0)
    owner_index = (shifted // REQ).astype(jnp.int32)
    within = (shifted % REQ).astype(jnp.int32)
    remote = requests[device, owner_index, within]
    columns = jnp.where(tile_slot < RB, device * RB + tile_slot, owner_index * RB + remote).astype(jnp.int32)
    rows_global = (device * RB + tile_row).astype(jnp.int32)
    live_mask = (position % TILES_DEV < tile_count[device]).astype(jnp.float32)

    def apply_matrix(vector):
        picked = vector[columns]
        products = jnp.einsum('tij,tkj->tki', tile_values, picked, precision=highest)
        products = products * live_mask[:, None, None]
        return jax.ops.segment_sum(products, rows_global, num_segments=vector.shape[0])
    beta_norm = jnp.sqrt(lax.optimization_barrier(jnp.sum(right_side * right_side, axis=(0, 2))) + epsilon)
    basis_list = [right_side / beta_norm[None, :, None]]
    hessenberg = jnp.zeros((right_side.shape[1], ITERS + 1, ITERS), jnp.float32)
    for column in range(ITERS):
        candidate = apply_matrix(basis_list[column])
        for earlier in range(column + 1):
            projection = lax.optimization_barrier(jnp.sum(candidate * basis_list[earlier], axis=(0, 2)))
            hessenberg = hessenberg.at[:, earlier, column].set(projection)
            candidate = candidate - projection[None, :, None] * basis_list[earlier]
        length = jnp.sqrt(lax.optimization_barrier(jnp.sum(candidate * candidate, axis=(0, 2))) + epsilon)
        hessenberg = hessenberg.at[:, column + 1, column].set(length)
        if column + 1 < ITERS:
            basis_list.append(candidate / length[None, :, None])
    weights = least_squares(hessenberg, beta_norm)
    stacked = jnp.stack(basis_list)
    solution = jnp.einsum('kj,jrki->rki', weights, stacked, precision=highest)
    return (solution, hessenberg)
```

```python
import functools

import jax
import jax.numpy as jnp
from jax import lax
from jax.experimental import pallas as pl
from jax.experimental.pallas import tpu as pltpu
from jax.sharding import PartitionSpec as P

ITERS = 3
MESH = pl.DeviceIdType.MESH
epsilon = 1e-06
f32 = jnp.float32
bf16 = jnp.bfloat16


def split(x):
    high = x.astype(bf16).astype(f32)
    return high, x - high


def dot(a, b):
    return lax.dot_general(a, b, (((1,), (0,)), ((), ())), preferred_element_type=f32)


def twice(x):
    return jnp.concatenate([x, x], axis=0)


def flip(value, mask, bits):
    result = 0
    for bit in range(bits):
        a = lax.rem(value // 2**bit, 2)
        b = mask // 2**bit % 2 if isinstance(mask, int) else lax.rem(mask // 2**bit, 2)
        result = result + (a + b - 2 * a * b) * 2**bit
    return result


def kernel(
    n,
    low,
    chunk,
    early,
    tile_hbm,
    row_hbm,
    count_hbm,
    slot_hbm,
    request_hbm,
    right_hbm,
    out_ref,
    hess_ref,
    tiles,
    parts,
    selector,
    row_ref,
    count_ref,
    slot_ref,
    request_ref,
    asked,
    outgoing,
    incoming,
    sums_out,
    sums_in,
    own,
    basis,
    table,
    highs,
    lows,
    tile_sem,
    load_sem,
    ask_send,
    ask_recv,
    send_sem,
    recv_sem,
    sums_send,
    sums_recv,
):
    me = lax.axis_index("rows")
    total, size, _ = tiles.shape
    _, height, _ = own.shape
    systems = outgoing.shape[2]
    blocks = height // systems
    rows = 2 * systems
    statics = blocks + n
    chunks = total // chunk
    far = n // low
    far_bits, low_bits = far.bit_length() - 1, low.bit_length() - 1
    group_of_me, place = me // low, lax.rem(me, low)
    beside = [flip(place, step, low_bits) for step in range(low)]

    def across(step):
        if far == 2**far_bits:
            return flip(group_of_me, step, far_bits) * low
        return lax.rem(group_of_me + step, far) * low

    home = group_of_me * low

    def far_first(body):
        def run(index, carry):
            group = across(far - 1 - index)
            for step in reversed(range(low)):
                body(group + beside[step])
            return carry

        lax.fori_loop(0, far - 1, run, 0, unroll=min(3, far - 1))
        for step in reversed(range(1, low)):
            body(home + beside[step])

    def remote(source, target, send, recv, peer):
        return pltpu.make_async_remote_copy(
            src_ref=source,
            dst_ref=target,
            send_sem=send,
            recv_sem=recv,
            device_id=(peer,),
            device_id_type=MESH,
        )

    barrier = pltpu.get_barrier_semaphore()
    far_first(
        lambda peer: pl.semaphore_signal(barrier, inc=1, device_id=(peer,), device_id_type=MESH)
    )

    def tile_copy(index):
        where = pl.ds(index * chunk, chunk)
        return pltpu.make_async_copy(tile_hbm.at[where], tiles.at[where], tile_sem.at[index])

    loads = [
        pltpu.make_async_copy(source, target, load_sem.at[index])
        for index, (source, target) in enumerate(
            [
                (request_hbm, request_ref),
                (row_hbm, row_ref),
                (count_hbm, count_ref),
                (slot_hbm, slot_ref),
                (right_hbm, own.at[0]),
            ]
        )
    ]
    for load in loads:
        load.start()
    for index in range(chunks):
        tile_copy(index).start()

    def split_chunk(index, carry):
        tile_copy(index).wait()

        def split_tile(offset, carry):
            tile = index * chunk + offset
            high, low_part = split(tiles[tile].T)
            parts[tile, 0:size, :] = high.astype(bf16)
            parts[tile, size : 2 * size, :] = low_part.astype(bf16)
            return carry

        return lax.fori_loop(0, chunk, split_tile, carry, unroll=4)

    lax.fori_loop(0, early, split_chunk, 0)
    pl.semaphore_wait(barrier, n - 1)
    for load in loads:
        load.wait()
    far_first(
        lambda peer: remote(request_ref, asked.at[me], ask_send, ask_recv, peer).start()
    )
    lax.fori_loop(early, chunks, split_chunk, 0)

    lane = lax.broadcasted_iota(jnp.int32, (1, total), 1)
    live_row = jnp.where(lane < count_ref[0], row_ref[...], blocks)
    wide = total * rows
    from_tile = lax.broadcasted_iota(jnp.int32, (total, wide), 0)
    to_column = lax.broadcasted_iota(jnp.int32, (total, wide), 1)
    expand = jnp.where(to_column // rows == from_tile, 1.0, 0.0).astype(bf16)
    row_of = dot(jnp.broadcast_to(live_row.astype(f32), (8, total)).astype(bf16), expand)[0:1]
    for pair in range(blocks // 2):
        k_row = lax.broadcasted_iota(jnp.int32, (rows, wide), 0)
        q_col = lax.broadcasted_iota(jnp.int32, (rows, wide), 1)
        block = (2 * pair + k_row // systems).astype(f32)
        fits = (k_row % systems == q_col % systems) & (
            jnp.broadcast_to(row_of, (rows, wide)) == block
        )
        selector[pl.ds(pair * rows, rows), :] = jnp.where(fits, 1.0, 0.0)

    sub = lax.broadcasted_iota(jnp.int32, (rows, size), 0)
    lanes = lax.broadcasted_iota(jnp.int32, (rows, size), 1)
    system_of = sub % systems

    def send_blocks(column):
        def send(peer):
            start = asked[peer, 0, me] * systems
            outgoing[column, peer] = own[column, pl.ds(start, systems), :]
            remote(
                outgoing.at[column, peer],
                incoming.at[column, me],
                send_sem.at[column],
                recv_sem.at[column, me],
                peer,
            ).start()

        far_first(send)

    def fold(x, y):
        product = (x * y).reshape(height // rows, rows, size)
        return jnp.sum(jnp.sum(product, axis=0), axis=1, keepdims=True)

    def send_sums(turn, sums):
        packed = jnp.zeros((rows, size), f32)
        for position, entry in enumerate(sums):
            packed = packed + jnp.where(lanes == rows * position + sub, entry, 0.0)
        packed = jnp.sum(packed, axis=0, keepdims=True)
        sums_out[turn] = packed
        sums_in[turn, me] = packed
        far_first(
            lambda peer: remote(
                sums_out.at[turn],
                sums_in.at[turn, me],
                sums_send.at[turn],
                sums_recv.at[turn],
                peer,
            ).start()
        )

    def all_sums(turn):
        others = pl.ds(0, n - 1)
        return remote(
            sums_in.at[turn, others],
            sums_in.at[turn, others],
            sums_send.at[turn],
            sums_recv.at[turn],
            home + beside[1],
        )

    def arrive_sums(turn, count):
        all_sums(turn).wait_recv()
        whole = jnp.sum(sums_in[turn], axis=0)
        whole = jnp.broadcast_to(whole, (rows, size))
        return [
            jnp.broadcast_to(
                jnp.sum(
                    jnp.where(
                        (lanes // rows == position) & (lanes % systems == system_of), whole, 0.0
                    ),
                    axis=1,
                    keepdims=True,
                ),
                (rows, size),
            )
            for position in range(count)
        ]

    def fill(slot, raw):
        high, rest = split(twice(raw))
        table[slot] = jnp.where(sub < systems, high, rest)

    def multiply(first, count):
        for pair in range(count // 2):
            both = []
            for side in range(2):
                tile, slot = first(2 * pair + side)
                x = table[slot].astype(bf16)
                both.append(dot(jnp.concatenate([x, x], axis=1), parts[tile]))
            y = jnp.concatenate(both, axis=0)
            high, rest = split(y)
            tile, _ = first(2 * pair)
            where = pl.ds(pl.multiple_of(tile * rows, 2 * rows), 2 * rows)
            highs[where, :] = high.astype(bf16)
            lows[where, :] = rest.astype(bf16)

    def near_tiles(column):
        for block in range(blocks):
            fill(block, own[column, pl.ds(block * systems, systems), :])
        multiply(lambda index: (index, index), blocks)

    def group_tiles(column, step):
        group = across(step)
        for index in range(low):
            fill(blocks + group + index, incoming[column, group + index])
        multiply(lambda index: (blocks + group + index, blocks + group + index), low)

    def arrive(column, step, skip):
        group = across(step)
        for index in range(skip, low):
            peer = group + beside[index]
            remote(
                outgoing.at[column, peer],
                incoming.at[column, peer],
                send_sem.at[column],
                recv_sem.at[column, peer],
                peer,
            ).wait_recv()

    def static_tiles(column):
        near_tiles(column)
        incoming[column, me] = own[column, pl.ds(request_ref[0, me] * systems, systems), :]
        arrive(column, 0, 1)
        group_tiles(column, 0)

        def run(step, carry):
            arrive(column, step, 0)
            group_tiles(column, step)
            return carry

        lax.fori_loop(1, far, run, 0, unroll=min(3, far - 1))

    def select():
        pick = selector[...].astype(bf16)
        return dot(pick, highs[...]) + dot(pick, lows[...])

    def spread(value):
        return jnp.tile(value, (height // rows, 1))

    zero = jnp.zeros((rows, size), f32)
    remote(asked.at[pl.ds(0, n - 1)], asked.at[pl.ds(0, n - 1)], ask_send, ask_recv, home).wait_recv()
    send_blocks(0)
    send_sums(0, [fold(own[0], own[0])])

    gram = {}
    triangle = []
    raw_columns = []
    rotations = []
    target = []
    coefficients = []
    extras = total - statics
    half = extras // 4 * 2

    def inner(i, j):
        return gram[(min(i, j), max(i, j))]

    def orthogonalize(column, summed):
        if column == 0:
            beta = jnp.sqrt(summed[0] + epsilon)
            scale = 1.0 / beta
            gram[(0, 0)] = summed[0] * scale * scale
            target.append(beta)
            return [], scale
        count = column
        values = []
        for i in range(count):
            value = summed[i]
            for earlier in range(i):
                value = value - values[earlier] * inner(earlier, i)
            values.append(value)
        residual = summed[count]
        for i in range(count):
            residual = residual - 2.0 * values[i] * summed[i]
        for i in range(count):
            for j in range(count):
                residual = residual + values[i] * values[j] * inner(i, j)
        residual = jnp.maximum(residual, 0.0)
        length = jnp.sqrt(residual + epsilon)
        scale = 1.0 / length
        if column < ITERS:
            for i in range(count):
                value = summed[i]
                for earlier in range(count):
                    value = value - values[earlier] * inner(earlier, i)
                gram[(i, count)] = value * scale
            gram[(count, count)] = residual * scale * scale
        raw_columns.append(values + [length])
        return values, scale

    for column in range(ITERS):
        static_tiles(column)
        multiply(lambda index: (statics + index, slot_ref[statics + index]), half)
        summed = arrive_sums(column, column + 1)
        values, scale = orthogonalize(column, summed)
        vector = own[column]
        for i, value in enumerate(values):
            vector = vector - spread(value) * basis[i]
        vector = vector * spread(scale)
        basis[column] = vector
        multiply(
            lambda index: (statics + half + index, slot_ref[statics + half + index]),
            extras - half,
        )
        candidate = select()
        for i, value in enumerate(values):
            candidate = candidate - spread(value) * own[i + 1]
        candidate = candidate * spread(scale)
        own[column + 1] = candidate
        if column + 1 < ITERS:
            send_blocks(column + 1)
        sums = [fold(candidate, basis[i]) for i in range(column + 1)]
        sums.append(fold(candidate, candidate))
        send_sums(column + 1, sums)
        if column >= 1:
            rotate(raw_columns[column - 1], rotations, triangle, target)

    summed = arrive_sums(ITERS, ITERS + 1)
    orthogonalize(ITERS, summed)
    rotate(raw_columns[ITERS - 1], rotations, triangle, target)
    weights = [None] * ITERS
    for column in reversed(range(ITERS)):
        value = target[column]
        for later in range(column + 1, ITERS):
            value = value - triangle[later][column] * weights[later]
        weights[column] = value / triangle[column][column]
    solved = spread(weights[0]) * basis[0]
    for i in range(1, ITERS):
        solved = solved + spread(weights[i]) * basis[i]
    out_ref[...] = solved
    for column in range(ITERS):
        picture = zero
        for i in range(column + 2):
            picture = jnp.where(lanes == i, raw_columns[column][i], picture)
        hess_ref[column] = picture[0:systems, 0 : ITERS + 1]
    others = pl.ds(0, n - 1)
    remote(asked.at[others], asked.at[others], ask_send, ask_recv, home).wait_send()
    for column in range(ITERS):
        remote(
            outgoing.at[column, others],
            incoming.at[column, others],
            send_sem.at[column],
            recv_sem.at[column, 0],
            home,
        ).wait_send()
    for turn in range(ITERS + 1):
        all_sums(turn).wait_send()


def rotate(column, rotations, triangle, target):
    column = list(column)
    for i, (cosine, sine) in enumerate(rotations):
        first, second = column[i], column[i + 1]
        column[i] = cosine * first + sine * second
        column[i + 1] = cosine * second - sine * first
    last = len(column) - 2
    first, second = column[last], column[last + 1]
    radius = jnp.sqrt(first * first + second * second)
    cosine, sine = first / radius, second / radius
    rotations.append((cosine, sine))
    column[last] = radius
    triangle.append(column[: last + 1])
    leading = target[last]
    target[last] = cosine * leading
    target.append(-sine * leading)


def hand_on(solved_ref, picture_ref, out_ref, hess_ref):
    out_ref[...] = solved_ref[...]
    hess_ref[...] = picture_ref[...]


def on_device(tile_values, tile_row, tile_slot, tile_count, requests, right_side):
    n = lax.axis_size("rows")
    total, size, _ = tile_values.shape
    blocks, systems, _ = right_side.shape
    rows = 2 * systems
    height = blocks * systems
    low = next(part for part in (8, 4, 2, 1) if n % part == 0)
    chunk = 16 if total % 16 == 0 else 1
    smem = pltpu.SMEM
    hbm = pl.BlockSpec(memory_space=pl.ANY)
    vmem = pl.BlockSpec(memory_space=pltpu.VMEM)
    dma = pltpu.SemaphoreType.DMA
    solved, picture = pl.pallas_call(
        functools.partial(kernel, n, low, chunk, min(3, total // chunk)),
        out_shape=(
            jax.ShapeDtypeStruct((height, size), f32),
            jax.ShapeDtypeStruct((ITERS, systems, ITERS + 1), f32),
        ),
        in_specs=[hbm] * 6,
        out_specs=(vmem, vmem),
        scratch_shapes=[
            pltpu.VMEM((total, size, size), f32),
            pltpu.VMEM((total, 2 * size, size), bf16),
            pltpu.VMEM((height, total * rows), f32),
            pltpu.VMEM((1, total), jnp.int32),
            smem((1,), jnp.int32),
            smem((total,), jnp.int32),
            smem((1, n), jnp.int32),
            smem((n, 1, n), jnp.int32),
            pltpu.VMEM((ITERS, n, systems, size), f32),
            pltpu.VMEM((ITERS, n, systems, size), f32),
            pltpu.VMEM((ITERS + 1, 1, size), f32),
            pltpu.VMEM((ITERS + 1, n, 1, size), f32),
            pltpu.VMEM((ITERS + 1, height, size), f32),
            pltpu.VMEM((ITERS, height, size), f32),
            pltpu.VMEM((blocks + n, rows, size), f32),
            pltpu.VMEM((total * rows, size), bf16),
            pltpu.VMEM((total * rows, size), bf16),
            dma((total // chunk,)),
            dma((5,)),
            dma,
            dma,
            dma((ITERS,)),
            dma((ITERS, n)),
            dma((ITERS + 1,)),
            dma((ITERS + 1,)),
        ],
        compiler_params=pltpu.CompilerParams(
            collective_id=0, has_side_effects=True, vmem_limit_bytes=60 * 1024 * 1024
        ),
        name="cycle",
    )(
        tile_values,
        tile_row.reshape(1, total),
        tile_count,
        tile_slot,
        requests.reshape(1, n),
        right_side.reshape(height, size),
    )
    solved, picture = pl.pallas_call(
        hand_on,
        out_shape=(
            jax.ShapeDtypeStruct(solved.shape, f32),
            jax.ShapeDtypeStruct(picture.shape, f32),
        ),
        in_specs=[vmem, vmem],
        out_specs=(vmem, vmem),
        name="hand_on",
    )(solved, picture)
    return solved.reshape(blocks, systems, size), jnp.transpose(picture, (1, 2, 0))


def solution(mesh):
    return jax.shard_map(
        on_device,
        mesh=mesh,
        in_specs=(
            P("rows", None, None),
            P("rows"),
            P("rows"),
            P("rows"),
            P("rows", None, None),
            P("rows", None, None),
        ),
        out_specs=(P("rows", None, None), P()),
        check_vma=False,
    )
```

```python
import functools

import jax
import jax.numpy as jnp
from jax import lax
from jax.experimental import pallas as pl
from jax.experimental.pallas import tpu as pltpu
from jax.sharding import PartitionSpec as P

ITERS = 3
LOADS = 5
MESH = pl.DeviceIdType.MESH
epsilon = 1e-06
f32 = jnp.float32
bf16 = jnp.bfloat16


def split(x):
    high = x.astype(bf16).astype(f32)
    return high, x - high


def dot(a, b):
    return lax.dot_general(a, b, (((1,), (0,)), ((), ())), preferred_element_type=f32)


def twice(x):
    return jnp.concatenate([x, x], axis=0)


def flip(value, mask, bits):
    result = 0
    for bit in range(bits):
        a = lax.rem(value // 2**bit, 2)
        b = mask // 2**bit % 2 if isinstance(mask, int) else lax.rem(mask // 2**bit, 2)
        result = result + (a + b - 2 * a * b) * 2**bit
    return result


def kernel(
    n,
    low,
    bounds,
    early,
    tile_hbm,
    row_hbm,
    count_hbm,
    slot_hbm,
    request_hbm,
    right_hbm,
    out_ref,
    hess_ref,
    tiles,
    parts,
    selector,
    row_ref,
    count_ref,
    slot_ref,
    request_ref,
    asked,
    outgoing,
    incoming,
    sums_out,
    sums_in,
    own,
    basis,
    table,
    products,
    solving,
    local_sem,
    ask_recv,
    recv_sem,
    sums_recv,
):
    me = lax.axis_index("rows")
    total, size, _ = tiles.shape
    _, height, _ = own.shape
    systems = outgoing.shape[2]
    blocks = height // systems
    rows = 2 * systems
    statics = blocks + n
    batch = size // rows
    far = n // low
    far_bits, low_bits = far.bit_length() - 1, low.bit_length() - 1
    group_of_me, place = me // low, lax.rem(me, low)
    beside = [flip(place, step, low_bits) for step in range(low)]

    def across(step):
        if far == 2**far_bits:
            return flip(group_of_me, step, far_bits) * low
        return lax.rem(group_of_me + step, far) * low

    home = group_of_me * low

    def far_first(body, top=far, bottom=0):
        def run(index, carry):
            group = across(top - 1 - index)
            for step in reversed(range(low)):
                body(group + beside[step])
            return carry

        stop = max(bottom, 1)
        if top - stop <= 3:
            for index in range(top - stop):
                run(index, 0)
        else:
            lax.fori_loop(0, top - stop, run, 0)
        if bottom == 0:
            for step in reversed(range(1, low)):
                body(home + beside[step])

    ask_send, send_sem, sums_send = (local_sem.at[index] for index in range(3))

    def remote(source, target, send, recv, peer):
        return pltpu.make_async_remote_copy(
            src_ref=source,
            dst_ref=target,
            send_sem=send,
            recv_sem=recv,
            device_id=(peer,),
            device_id_type=MESH,
        )

    tile_copies = [
        pltpu.make_async_copy(
            tile_hbm.at[pl.ds(begin, end - begin)],
            tiles.at[pl.ds(begin, end - begin)],
            local_sem.at[LOADS + index],
        )
        for index, (begin, end) in enumerate(zip(bounds[:-1], bounds[1:]))
    ]
    tile_copies[0].start()
    barrier = pltpu.get_barrier_semaphore()
    far_first(
        lambda peer: pl.semaphore_signal(barrier, inc=1, device_id=(peer,), device_id_type=MESH)
    )

    loads = [
        pltpu.make_async_copy(source, target, local_sem.at[index])
        for index, (source, target) in enumerate(
            [
                (request_hbm, request_ref),
                (row_hbm, row_ref),
                (count_hbm, count_ref),
                (slot_hbm, slot_ref),
                (right_hbm, own.at[0]),
            ]
        )
    ]
    for load in loads:
        load.start()
    for copy in tile_copies[1:]:
        copy.start()

    def split_tiles(index):
        tile_copies[index].wait()

        def split_tile(tile, carry):
            high, low_part = split(tiles[tile].T)
            parts[tile, 0:size, :] = high.astype(bf16)
            parts[tile, size : 2 * size, :] = low_part.astype(bf16)
            return carry

        lax.fori_loop(bounds[index], bounds[index + 1], split_tile, 0, unroll=4)

    for index in range(early):
        split_tiles(index)
    pl.semaphore_wait(barrier, n - 1)
    for load in loads:
        load.wait()
    far_first(
        lambda peer: remote(request_ref, asked.at[me], ask_send, ask_recv, peer).start()
    )
    for index in range(early, len(tile_copies)):
        split_tiles(index)

    lane = lax.broadcasted_iota(jnp.int32, (1, total), 1)
    live_row = jnp.where(lane < count_ref[0], row_ref[...], blocks)
    wide = total * rows
    from_tile = lax.broadcasted_iota(jnp.int32, (total, wide), 0)
    to_column = lax.broadcasted_iota(jnp.int32, (total, wide), 1)
    expand = jnp.where(to_column // rows == from_tile, 1.0, 0.0).astype(bf16)
    row_of = dot(jnp.broadcast_to(live_row.astype(f32), (8, total)).astype(bf16), expand)[0:1]
    k_row = lax.broadcasted_iota(jnp.int32, (height, size), 0)
    q_col = lax.broadcasted_iota(jnp.int32, (height, size), 1)
    same_system = k_row % systems == q_col % systems
    block = (k_row // systems).astype(f32)
    for part in range(total // batch):
        here = row_of[:, part * size : (part + 1) * size]
        fits = same_system & (jnp.broadcast_to(here, (height, size)) == block)
        mask = jnp.where(fits, 1.0, 0.0).astype(bf16)
        selector[part, :, 0:size] = mask
        selector[part, :, size : 2 * size] = mask

    sub = lax.broadcasted_iota(jnp.int32, (rows, size), 0)
    lanes = lax.broadcasted_iota(jnp.int32, (rows, size), 1)
    system_of = sub % systems

    def send_blocks(column, top, bottom):
        def send(peer):
            start = asked[peer, 0, me] * systems
            outgoing[column, peer] = own[column, pl.ds(start, systems), :]
            remote(
                outgoing.at[column, peer],
                incoming.at[column, me],
                send_sem,
                recv_sem.at[column % 2, group_of_me],
                peer,
            ).start()

        far_first(send, top, bottom)

    def fold(x, y):
        product = (x * y).reshape(height // rows, rows, size)
        return jnp.sum(jnp.sum(product, axis=0), axis=1, keepdims=True)

    def send_sums(turn, sums):
        packed = jnp.zeros((rows, size), f32)
        for position, entry in enumerate(sums):
            packed = packed + jnp.where(lanes == rows * position + sub, entry, 0.0)
        packed = jnp.sum(packed, axis=0, keepdims=True)
        sums_out[turn] = packed
        sums_in[turn, me] = packed
        far_first(
            lambda peer: remote(
                sums_out.at[turn],
                sums_in.at[turn, me],
                sums_send,
                sums_recv.at[turn % 2],
                peer,
            ).start()
        )

    def all_sums(turn):
        others = pl.ds(0, n - 1)
        return remote(
            sums_in.at[turn, others],
            sums_in.at[turn, others],
            sums_send,
            sums_recv.at[turn % 2],
            home + beside[1],
        )

    def arrive_sums(turn, count):
        all_sums(turn).wait_recv()
        whole = jnp.sum(sums_in[turn], axis=0)
        whole = jnp.broadcast_to(whole, (rows, size))
        return [
            jnp.broadcast_to(
                jnp.sum(
                    jnp.where(
                        (lanes // rows == position) & (lanes % systems == system_of), whole, 0.0
                    ),
                    axis=1,
                    keepdims=True,
                ),
                (rows, size),
            )
            for position in range(count)
        ]

    def fill(slot, raw):
        high, rest = split(twice(raw))
        table[slot] = jnp.where(sub < systems, high, rest)

    def multiply(first, count):
        for pair in range(count // 2):
            both = []
            for side in range(2):
                tile, slot = first(2 * pair + side)
                x = table[slot].astype(bf16)
                both.append(dot(jnp.concatenate([x, x], axis=1), parts[tile]))
            y = jnp.concatenate(both, axis=0)
            high, rest = split(y)
            tile, _ = first(2 * pair)
            if isinstance(tile, int):
                part, start = tile // batch, tile % batch * rows
            else:
                part, start = tile // batch, pl.multiple_of(lax.rem(tile, batch) * rows, 2 * rows)
            products[part, pl.ds(start, 2 * rows), :] = high.astype(bf16)
            products[part, pl.ds(size + start, 2 * rows), :] = rest.astype(bf16)

    def near_tiles(column):
        for block in range(blocks):
            fill(block, own[column, pl.ds(block * systems, systems), :])
        multiply(lambda index: (index, index), blocks)

    def group_tiles(column, group):
        for index in range(low):
            fill(blocks + group + index, incoming[column, group + index])
        multiply(lambda index: (blocks + group + index, blocks + group + index), low)

    def arrive(column, step):
        group = across(step)
        count = low - 1 if isinstance(step, int) and step == 0 else low
        remote(
            outgoing.at[column, pl.ds(group, count)],
            incoming.at[column, pl.ds(group, count)],
            send_sem,
            recv_sem.at[column % 2, group // low],
            home + beside[1],
        ).wait_recv()

    def static_tiles(column):
        near_tiles(column)
        incoming[column, me] = own[column, pl.ds(request_ref[0, me] * systems, systems), :]
        arrive(column, 0)
        group_tiles(column, home)

        def run(step, carry):
            arrive(column, step)
            group_tiles(column, across(step))
            return carry

        if far <= 4:
            for step in range(1, far - 1):
                run(step, 0)
        else:
            lax.fori_loop(1, far - 1, run, 0)
        arrive(column, far - 1)

    def select():
        result = dot(selector[0], products[0])
        for part in range(1, total // batch):
            result = result + dot(selector[part], products[part])
        return result

    def spread(value):
        return jnp.tile(value, (height // rows, 1))

    zero = jnp.zeros((rows, size), f32)
    remote(asked.at[pl.ds(0, n - 1)], asked.at[pl.ds(0, n - 1)], ask_send, ask_recv, home + beside[1]).wait_recv()
    middle = far // 2
    send_blocks(0, far, middle)
    send_sums(0, [fold(own[0], own[0])])
    send_blocks(0, middle, 0)

    gram = {}
    triangle = []
    raw_columns = []
    rotations = []
    target = []
    coefficients = []
    extras = total - statics

    def inner(i, j):
        return gram[(min(i, j), max(i, j))]

    def orthogonalize(column, summed):
        if column == 0:
            beta = jnp.sqrt(summed[0] + epsilon)
            scale = 1.0 / beta
            gram[(0, 0)] = summed[0] * scale * scale
            target.append(beta)
            return [], scale
        count = column
        values, square = project(column, summed)
        length = jnp.sqrt(square)
        scale = 1.0 / length
        for i in range(count):
            value = summed[i]
            for earlier in range(count):
                value = value - values[earlier] * inner(earlier, i)
            gram[(i, count)] = value * scale
        gram[(count, count)] = (square - epsilon) * scale * scale
        raw_columns.append(values + [length])
        return values, scale

    def project(count, summed):
        values = []
        for i in range(count):
            value = summed[i]
            for earlier in range(i):
                value = value - values[earlier] * inner(earlier, i)
            values.append(value)
        residual = summed[count]
        for i in range(count):
            residual = residual - 2.0 * values[i] * summed[i]
        for i in range(count):
            for j in range(count):
                residual = residual + values[i] * values[j] * inner(i, j)
        return values, jnp.maximum(residual, 0.0) + epsilon

    for column in range(ITERS):
        static_tiles(column)
        group_tiles(column, across(far - 1))
        multiply(lambda index: (statics + index, slot_ref[statics + index]), extras)
        summed = arrive_sums(column, column + 1)
        values, scale = orthogonalize(column, summed)
        vector = own[column]
        for i, value in enumerate(values):
            vector = vector - spread(value) * basis[i]
        vector = vector * spread(scale)
        basis[column] = vector
        candidate = select()
        for i, value in enumerate(values):
            candidate = candidate - spread(value) * own[i + 1]
        candidate = candidate * spread(scale)
        own[column + 1] = candidate
        if column + 1 < ITERS:
            send_blocks(column + 1, far, middle)
        sums = [fold(candidate, basis[i]) for i in range(column + 1)]
        sums.append(fold(candidate, candidate))
        send_sums(column + 1, sums)
        if column + 1 < ITERS:
            send_blocks(column + 1, middle, 0)
        if column >= 1:
            rotate(raw_columns[column - 1], rotations, triangle, target)

    last = ITERS - 1
    inverse = [1.0 / triangle[column][column] for column in range(last)]

    def back(entries):
        found = [None] * last
        for column in reversed(range(last)):
            value = entries[column]
            for later in range(column + 1, last):
                value = value - triangle[later][column] * found[later]
            found[column] = value * inverse[column]
        return found

    before = back(target[0:last])
    start = spread(before[0]) * basis[0]
    for i in range(1, last):
        start = start + spread(before[i]) * basis[i]
    solving[...] = start
    summed = arrive_sums(ITERS, ITERS + 1)
    values, square = project(ITERS, summed)
    entries = list(values)
    for i, (cosine, sine) in enumerate(rotations):
        first, second = entries[i], entries[i + 1]
        entries[i] = cosine * first + sine * second
        entries[i + 1] = cosine * second - sine * first
    lead = entries[last]
    weight = lead * target[last] / (lead * lead + square)
    along = back(entries[0:last])
    solved = solving[...] + spread(weight) * basis[last]
    for i in range(last):
        solved = solved - spread(weight * along[i]) * basis[i]
    out_ref[...] = solved
    raw_columns.append(values + [jnp.sqrt(square)])
    for column in range(ITERS):
        picture = zero
        for i in range(column + 2):
            picture = jnp.where(lanes == i, raw_columns[column][i], picture)
        hess_ref[column] = picture[0:systems, 0 : ITERS + 1]
    others = pl.ds(0, n - 1)
    peer = home + beside[1]
    remote(asked.at[others], asked.at[others], ask_send, ask_recv, peer).wait_send()
    remote(
        outgoing.at[:, others], incoming.at[:, others], send_sem, recv_sem.at[0, 0], peer
    ).wait_send()
    remote(
        sums_in.at[:, others], sums_in.at[:, others], sums_send, sums_recv.at[0], peer
    ).wait_send()


def rotate(column, rotations, triangle, target):
    column = list(column)
    for i, (cosine, sine) in enumerate(rotations):
        first, second = column[i], column[i + 1]
        column[i] = cosine * first + sine * second
        column[i + 1] = cosine * second - sine * first
    last = len(column) - 2
    first, second = column[last], column[last + 1]
    radius = jnp.sqrt(first * first + second * second)
    cosine, sine = first / radius, second / radius
    rotations.append((cosine, sine))
    column[last] = radius
    triangle.append(column[: last + 1])
    leading = target[last]
    target[last] = cosine * leading
    target.append(-sine * leading)


def hand_on(solved_ref, picture_ref, out_ref, hess_ref, sem):
    copies = [
        pltpu.make_async_copy(solved_ref, out_ref, sem.at[0]),
        pltpu.make_async_copy(picture_ref, hess_ref, sem.at[1]),
    ]
    for copy in copies:
        copy.start()
    for copy in copies:
        copy.wait()


def on_device(tile_values, tile_row, tile_slot, tile_count, requests, right_side):
    n = lax.axis_size("rows")
    total, size, _ = tile_values.shape
    blocks, systems, _ = right_side.shape
    rows = 2 * systems
    height = blocks * systems
    low = next(part for part in (8, 4, 2, 1) if n % part == 0)
    begin = blocks + blocks
    bounds = (0, blocks, begin, (begin + total) // 2, total)
    smem = pltpu.SMEM
    hbm = pl.BlockSpec(memory_space=pl.ANY)
    vmem = pl.BlockSpec(memory_space=pltpu.VMEM)
    dma = pltpu.SemaphoreType.DMA
    solved, picture = pl.pallas_call(
        functools.partial(kernel, n, low, bounds, 2),
        out_shape=(
            pltpu.VMEM((height, size), f32),
            pltpu.VMEM((ITERS, systems, ITERS + 1), f32),
        ),
        in_specs=[hbm] * 6,
        out_specs=(vmem, vmem),
        scratch_shapes=[
            pltpu.VMEM((total, size, size), f32),
            pltpu.VMEM((total, 2 * size, size), bf16),
            pltpu.VMEM((total * rows // size, height, 2 * size), bf16),
            pltpu.VMEM((1, total), jnp.int32),
            smem((1,), jnp.int32),
            smem((total,), jnp.int32),
            smem((1, n), jnp.int32),
            smem((n, 1, n), jnp.int32),
            pltpu.VMEM((ITERS, n, systems, size), f32),
            pltpu.VMEM((ITERS, n, systems, size), f32),
            pltpu.VMEM((ITERS + 1, 1, size), f32),
            pltpu.VMEM((ITERS + 1, n, 1, size), f32),
            pltpu.VMEM((ITERS + 1, height, size), f32),
            pltpu.VMEM((ITERS, height, size), f32),
            pltpu.VMEM((blocks + n, rows, size), f32),
            pltpu.VMEM((total * rows // size, 2 * size, size), bf16),
            pltpu.VMEM((height, size), f32),
            dma((LOADS + len(bounds) - 1,)),
            dma,
            dma((2, n // low)),
            dma((2,)),
        ],
        compiler_params=pltpu.CompilerParams(
            collective_id=0, has_side_effects=True, vmem_limit_bytes=60 * 1024 * 1024
        ),
        name="cycle",
    )(
        tile_values,
        tile_row.reshape(1, total),
        tile_count,
        tile_slot,
        requests.reshape(1, n),
        right_side.reshape(height, size),
    )
    solved, picture = pl.pallas_call(
        hand_on,
        out_shape=(
            jax.ShapeDtypeStruct(solved.shape, f32),
            jax.ShapeDtypeStruct(picture.shape, f32),
        ),
        in_specs=[hbm, hbm],
        out_specs=(hbm, hbm),
        scratch_shapes=[dma((2,))],
        compiler_params=pltpu.CompilerParams(vmem_limit_bytes=1 << 20),
        name="hand_on",
    )(solved, picture)
    return solved.reshape(blocks, systems, size), jnp.transpose(picture, (1, 2, 0))


def solution(mesh):
    return jax.shard_map(
        on_device,
        mesh=mesh,
        in_specs=(
            P("rows", None, None),
            P("rows"),
            P("rows"),
            P("rows"),
            P("rows", None, None),
            P("rows", None, None),
        ),
        out_specs=(P("rows", None, None), P()),
        check_vma=False,
    )
```

```python
import functools

import jax
import jax.numpy as jnp
from jax import lax
from jax.experimental import pallas as pl
from jax.experimental.pallas import tpu as pltpu
from jax.sharding import PartitionSpec as P

ITERS = 3
LOADS = 5
MESH = pl.DeviceIdType.MESH
epsilon = 1e-06
f32 = jnp.float32
bf16 = jnp.bfloat16


def split(x):
    high = x.astype(bf16).astype(f32)
    return high, x - high


def dot(a, b):
    return lax.dot_general(a, b, (((1,), (0,)), ((), ())), preferred_element_type=f32)


def twice(x):
    return jnp.concatenate([x, x], axis=0)


def flip(value, mask, bits):
    result = 0
    for bit in range(bits):
        a = lax.rem(value // 2**bit, 2)
        b = mask // 2**bit % 2 if isinstance(mask, int) else lax.rem(mask // 2**bit, 2)
        result = result + (a + b - 2 * a * b) * 2**bit
    return result


def kernel(
    n,
    low,
    bounds,
    early,
    tile_hbm,
    row_hbm,
    count_hbm,
    slot_hbm,
    request_hbm,
    right_hbm,
    out_ref,
    hess_ref,
    tiles,
    parts,
    selector,
    row_ref,
    count_ref,
    slot_ref,
    request_ref,
    asked,
    outgoing,
    incoming,
    sums_out,
    sums_in,
    own,
    basis,
    table,
    products,
    solving,
    local_sem,
    ask_recv,
    recv_sem,
    sums_recv,
):
    me = lax.axis_index("rows")
    total, size, _ = tiles.shape
    _, height, _ = own.shape
    systems = outgoing.shape[2]
    blocks = height // systems
    rows = 2 * systems
    statics = blocks + n
    batch = size // rows
    far = n // low
    far_bits, low_bits = far.bit_length() - 1, low.bit_length() - 1
    group_of_me, place = me // low, lax.rem(me, low)
    beside = [flip(place, step, low_bits) for step in range(low)]

    quarter = group_of_me * 4 // far
    swap = jnp.where((quarter == 1) | (quarter == 2), 1, 0) if far % 4 == 0 else 0

    def across(step):
        if far % 4 == 0 and isinstance(step, int) and step >= far - 2:
            step = step - swap if step == far - 1 else step + swap
        if far == 2**far_bits:
            return flip(group_of_me, step, far_bits) * low
        return lax.rem(group_of_me + step, far) * low

    home = group_of_me * low

    def far_first(body, top=far, bottom=0):
        def run(index, carry):
            group = across(top - 1 - index)
            for step in reversed(range(low)):
                body(group + beside[step])
            return carry

        stop = max(bottom, 1)
        if top - stop <= 3:
            for index in range(top - stop):
                run(index, 0)
        else:
            lax.fori_loop(0, top - stop, run, 0)
        if bottom == 0:
            for step in reversed(range(1, low)):
                body(home + beside[step])

    ask_send, send_sem, sums_send = (local_sem.at[index] for index in range(3))

    def remote(source, target, send, recv, peer):
        return pltpu.make_async_remote_copy(
            src_ref=source,
            dst_ref=target,
            send_sem=send,
            recv_sem=recv,
            device_id=(peer,),
            device_id_type=MESH,
        )

    tile_copies = [
        pltpu.make_async_copy(
            tile_hbm.at[pl.ds(begin, end - begin)],
            tiles.at[pl.ds(begin, end - begin)],
            local_sem.at[LOADS + index],
        )
        for index, (begin, end) in enumerate(zip(bounds[:-1], bounds[1:]))
    ]
    barrier = pltpu.get_barrier_semaphore()
    far_first(
        lambda peer: pl.semaphore_signal(barrier, inc=1, device_id=(peer,), device_id_type=MESH)
    )

    loads = [
        pltpu.make_async_copy(source, target, local_sem.at[index])
        for index, (source, target) in enumerate(
            [
                (request_hbm, request_ref),
                (row_hbm, row_ref),
                (count_hbm, count_ref),
                (slot_hbm, slot_ref),
                (right_hbm, own.at[0]),
            ]
        )
    ]
    tile_copies[0].start()
    for load in loads:
        load.start()
    for copy in tile_copies[1:]:
        copy.start()

    def split_tiles(index):
        tile_copies[index].wait()

        def split_tile(tile, carry):
            high, low_part = split(tiles[tile].T)
            parts[tile, 0:size, :] = high.astype(bf16)
            parts[tile, size : 2 * size, :] = low_part.astype(bf16)
            return carry

        lax.fori_loop(bounds[index], bounds[index + 1], split_tile, 0, unroll=4)

    for index in range(early):
        split_tiles(index)
    pl.semaphore_wait(barrier, n - 1)
    loads[0].wait()
    far_first(
        lambda peer: remote(request_ref, asked.at[me], ask_send, ask_recv, peer).start()
    )
    for load in loads[1:]:
        load.wait()
    for index in range(early, len(tile_copies)):
        split_tiles(index)

    lane = lax.broadcasted_iota(jnp.int32, (1, total), 1)
    live_row = jnp.where(lane < count_ref[0], row_ref[...], blocks)
    wide = total * rows
    from_tile = lax.broadcasted_iota(jnp.int32, (total, wide), 0)
    to_column = lax.broadcasted_iota(jnp.int32, (total, wide), 1)
    expand = jnp.where(to_column // rows == from_tile, 1.0, 0.0).astype(bf16)
    row_of = dot(jnp.broadcast_to(live_row.astype(f32), (8, total)).astype(bf16), expand)[0:1]
    k_row = lax.broadcasted_iota(jnp.int32, (height, size), 0)
    q_col = lax.broadcasted_iota(jnp.int32, (height, size), 1)
    same_system = k_row % systems == q_col % systems
    block = (k_row // systems).astype(f32)
    for part in range(total // batch):
        here = row_of[:, part * size : (part + 1) * size]
        fits = same_system & (jnp.broadcast_to(here, (height, size)) == block)
        mask = jnp.where(fits, 1.0, 0.0).astype(bf16)
        selector[part, :, 0:size] = mask
        selector[part, :, size : 2 * size] = mask

    sub = lax.broadcasted_iota(jnp.int32, (rows, size), 0)
    lanes = lax.broadcasted_iota(jnp.int32, (rows, size), 1)
    system_of = sub % systems

    def send_blocks(column, top, bottom):
        def send(peer):
            start = asked[peer, 0, me] * systems
            outgoing[column, peer] = own[column, pl.ds(start, systems), :]
            remote(
                outgoing.at[column, peer],
                incoming.at[column, me],
                send_sem,
                recv_sem.at[column % 2, group_of_me],
                peer,
            ).start()

        far_first(send, top, bottom)

    def fold(x, y):
        product = (x * y).reshape(height // rows, rows, size)
        return jnp.sum(jnp.sum(product, axis=0), axis=1, keepdims=True)

    def send_sums(turn, sums):
        packed = jnp.zeros((rows, size), f32)
        for position, entry in enumerate(sums):
            packed = packed + jnp.where(lanes == rows * position + sub, entry, 0.0)
        packed = jnp.sum(packed, axis=0, keepdims=True)
        sums_out[turn] = packed
        sums_in[turn, me] = packed
        far_first(
            lambda peer: remote(
                sums_out.at[turn],
                sums_in.at[turn, me],
                sums_send,
                sums_recv.at[turn % 2],
                peer,
            ).start()
        )

    def all_sums(turn):
        others = pl.ds(0, n - 1)
        return remote(
            sums_in.at[turn, others],
            sums_in.at[turn, others],
            sums_send,
            sums_recv.at[turn % 2],
            home + beside[1],
        )

    def arrive_sums(turn, count):
        all_sums(turn).wait_recv()
        whole = jnp.sum(sums_in[turn], axis=0)
        whole = jnp.broadcast_to(whole, (rows, size))
        return [
            jnp.broadcast_to(
                jnp.sum(
                    jnp.where(
                        (lanes // rows == position) & (lanes % systems == system_of), whole, 0.0
                    ),
                    axis=1,
                    keepdims=True,
                ),
                (rows, size),
            )
            for position in range(count)
        ]

    def fill(slot, raw):
        high, rest = split(twice(raw))
        table[slot] = jnp.where(sub < systems, high, rest)

    def multiply(first, count):
        for pair in range(count // 2):
            both = []
            for side in range(2):
                tile, slot = first(2 * pair + side)
                x = table[slot].astype(bf16)
                both.append(dot(jnp.concatenate([x, x], axis=1), parts[tile]))
            y = jnp.concatenate(both, axis=0)
            high, rest = split(y)
            tile, _ = first(2 * pair)
            if isinstance(tile, int):
                part, start = tile // batch, tile % batch * rows
            else:
                part, start = tile // batch, pl.multiple_of(lax.rem(tile, batch) * rows, 2 * rows)
            products[part, pl.ds(start, 2 * rows), :] = high.astype(bf16)
            products[part, pl.ds(size + start, 2 * rows), :] = rest.astype(bf16)

    def near_tiles(column):
        for block in range(blocks):
            fill(block, own[column, pl.ds(block * systems, systems), :])
        multiply(lambda index: (index, index), blocks)

    def group_tiles(column, group):
        for index in range(low):
            fill(blocks + group + index, incoming[column, group + index])
        multiply(lambda index: (blocks + group + index, blocks + group + index), low)

    def arrive(column, step):
        group = across(step)
        count = low - 1 if isinstance(step, int) and step == 0 else low
        remote(
            outgoing.at[column, pl.ds(group, count)],
            incoming.at[column, pl.ds(group, count)],
            send_sem,
            recv_sem.at[column % 2, group // low],
            home + beside[1],
        ).wait_recv()

    def static_tiles(column):
        near_tiles(column)
        incoming[column, me] = own[column, pl.ds(request_ref[0, me] * systems, systems), :]
        arrive(column, 0)
        group_tiles(column, home)

        def run(step, carry):
            arrive(column, step)
            group_tiles(column, across(step))
            return carry

        if far <= 4:
            for step in range(1, far - 1):
                run(step, 0)
        else:
            lax.fori_loop(1, far - 1, run, 0)
        arrive(column, far - 1)

    def select():
        result = dot(selector[0], products[0])
        for part in range(1, total // batch):
            result = result + dot(selector[part], products[part])
        return result

    def spread(value):
        return jnp.tile(value, (height // rows, 1))

    zero = jnp.zeros((rows, size), f32)
    remote(asked.at[pl.ds(0, n - 1)], asked.at[pl.ds(0, n - 1)], ask_send, ask_recv, home + beside[1]).wait_recv()
    send_blocks(0, far, 0)
    send_sums(0, [fold(own[0], own[0])])

    gram = {}
    triangle = []
    raw_columns = []
    rotations = []
    target = []
    coefficients = []
    extras = total - statics

    def inner(i, j):
        return gram[(min(i, j), max(i, j))]

    def orthogonalize(column, summed):
        if column == 0:
            beta = jnp.sqrt(summed[0] + epsilon)
            scale = 1.0 / beta
            gram[(0, 0)] = summed[0] * scale * scale
            target.append(beta)
            return [], scale
        count = column
        values, square = project(column, summed)
        length = jnp.sqrt(square)
        scale = 1.0 / length
        for i in range(count):
            value = summed[i]
            for earlier in range(count):
                value = value - values[earlier] * inner(earlier, i)
            gram[(i, count)] = value * scale
        gram[(count, count)] = (square - epsilon) * scale * scale
        raw_columns.append(values + [length])
        return values, scale

    def project(count, summed):
        values = []
        for i in range(count):
            value = summed[i]
            for earlier in range(i):
                value = value - values[earlier] * inner(earlier, i)
            values.append(value)
        residual = summed[count]
        for i in range(count):
            residual = residual - 2.0 * values[i] * summed[i]
        for i in range(count):
            for j in range(count):
                residual = residual + values[i] * values[j] * inner(i, j)
        return values, jnp.maximum(residual, 0.0) + epsilon

    for column in range(ITERS):
        static_tiles(column)
        group_tiles(column, across(far - 1))
        multiply(lambda index: (statics + index, slot_ref[statics + index]), extras)
        summed = arrive_sums(column, column + 1)
        values, scale = orthogonalize(column, summed)
        vector = own[column]
        for i, value in enumerate(values):
            vector = vector - spread(value) * basis[i]
        vector = vector * spread(scale)
        basis[column] = vector
        candidate = select()
        for i, value in enumerate(values):
            candidate = candidate - spread(value) * own[i + 1]
        candidate = candidate * spread(scale)
        own[column + 1] = candidate
        if column + 1 < ITERS:
            send_blocks(column + 1, far, 0)
        sums = [fold(candidate, basis[i]) for i in range(column + 1)]
        sums.append(fold(candidate, candidate))
        send_sums(column + 1, sums)
        if column >= 1:
            rotate(raw_columns[column - 1], rotations, triangle, target)

    last = ITERS - 1
    inverse = [1.0 / triangle[column][column] for column in range(last)]

    def back(entries):
        found = [None] * last
        for column in reversed(range(last)):
            value = entries[column]
            for later in range(column + 1, last):
                value = value - triangle[later][column] * found[later]
            found[column] = value * inverse[column]
        return found

    before = back(target[0:last])
    start = spread(before[0]) * basis[0]
    for i in range(1, last):
        start = start + spread(before[i]) * basis[i]
    solving[...] = start
    summed = arrive_sums(ITERS, ITERS + 1)
    values, square = project(ITERS, summed)
    entries = list(values)
    for i, (cosine, sine) in enumerate(rotations):
        first, second = entries[i], entries[i + 1]
        entries[i] = cosine * first + sine * second
        entries[i + 1] = cosine * second - sine * first
    lead = entries[last]
    weight = lead * target[last] / (lead * lead + square)
    along = back(entries[0:last])
    solved = solving[...] + spread(weight) * basis[last]
    for i in range(last):
        solved = solved - spread(weight * along[i]) * basis[i]
    out_ref[...] = solved
    raw_columns.append(values + [jnp.sqrt(square)])
    for column in range(ITERS):
        picture = zero
        for i in range(column + 2):
            picture = jnp.where(lanes == i, raw_columns[column][i], picture)
        hess_ref[column] = picture[0:systems, 0 : ITERS + 1]
    others = pl.ds(0, n - 1)
    peer = home + beside[1]
    remote(asked.at[others], asked.at[others], ask_send, ask_recv, peer).wait_send()
    remote(
        outgoing.at[:, others], incoming.at[:, others], send_sem, recv_sem.at[0, 0], peer
    ).wait_send()
    remote(
        sums_in.at[:, others], sums_in.at[:, others], sums_send, sums_recv.at[0], peer
    ).wait_send()


def rotate(column, rotations, triangle, target):
    column = list(column)
    for i, (cosine, sine) in enumerate(rotations):
        first, second = column[i], column[i + 1]
        column[i] = cosine * first + sine * second
        column[i + 1] = cosine * second - sine * first
    last = len(column) - 2
    first, second = column[last], column[last + 1]
    radius = jnp.sqrt(first * first + second * second)
    cosine, sine = first / radius, second / radius
    rotations.append((cosine, sine))
    column[last] = radius
    triangle.append(column[: last + 1])
    leading = target[last]
    target[last] = cosine * leading
    target.append(-sine * leading)


def hand_on(solved_ref, picture_ref, out_ref, hess_ref, sem):
    copies = [
        pltpu.make_async_copy(solved_ref, out_ref, sem.at[0]),
        pltpu.make_async_copy(picture_ref, hess_ref, sem.at[1]),
    ]
    for copy in copies:
        copy.start()
    for copy in copies:
        copy.wait()


def on_device(tile_values, tile_row, tile_slot, tile_count, requests, right_side):
    n = lax.axis_size("rows")
    total, size, _ = tile_values.shape
    blocks, systems, _ = right_side.shape
    rows = 2 * systems
    height = blocks * systems
    low = next(part for part in (8, 4, 2, 1) if n % part == 0)
    begin = blocks + blocks
    bounds = (0, blocks, begin, (begin + total) // 2, total)
    smem = pltpu.SMEM
    hbm = pl.BlockSpec(memory_space=pl.ANY)
    vmem = pl.BlockSpec(memory_space=pltpu.VMEM)
    dma = pltpu.SemaphoreType.DMA
    solved, picture = pl.pallas_call(
        functools.partial(kernel, n, low, bounds, 2),
        out_shape=(
            pltpu.VMEM((height, size), f32),
            pltpu.VMEM((ITERS, systems, ITERS + 1), f32),
        ),
        in_specs=[hbm] * 6,
        out_specs=(vmem, vmem),
        scratch_shapes=[
            pltpu.VMEM((total, size, size), f32),
            pltpu.VMEM((total, 2 * size, size), bf16),
            pltpu.VMEM((total * rows // size, height, 2 * size), bf16),
            pltpu.VMEM((1, total), jnp.int32),
            smem((1,), jnp.int32),
            smem((total,), jnp.int32),
            smem((1, n), jnp.int32),
            smem((n, 1, n), jnp.int32),
            pltpu.VMEM((ITERS, n, systems, size), f32),
            pltpu.VMEM((ITERS, n, systems, size), f32),
            pltpu.VMEM((ITERS + 1, 1, size), f32),
            pltpu.VMEM((ITERS + 1, n, 1, size), f32),
            pltpu.VMEM((ITERS + 1, height, size), f32),
            pltpu.VMEM((ITERS, height, size), f32),
            pltpu.VMEM((blocks + n, rows, size), f32),
            pltpu.VMEM((total * rows // size, 2 * size, size), bf16),
            pltpu.VMEM((height, size), f32),
            dma((LOADS + len(bounds) - 1,)),
            dma,
            dma((2, n // low)),
            dma((2,)),
        ],
        compiler_params=pltpu.CompilerParams(
            collective_id=0, has_side_effects=True, vmem_limit_bytes=60 * 1024 * 1024
        ),
        name="cycle",
    )(
        tile_values,
        tile_row.reshape(1, total),
        tile_count,
        tile_slot,
        requests.reshape(1, n),
        right_side.reshape(height, size),
    )
    solved, picture = pl.pallas_call(
        hand_on,
        out_shape=(
            jax.ShapeDtypeStruct(solved.shape, f32),
            jax.ShapeDtypeStruct(picture.shape, f32),
        ),
        in_specs=[hbm, hbm],
        out_specs=(hbm, hbm),
        scratch_shapes=[dma((2,))],
        compiler_params=pltpu.CompilerParams(vmem_limit_bytes=1 << 20),
        name="hand_on",
    )(solved, picture)
    return solved.reshape(blocks, systems, size), jnp.transpose(picture, (1, 2, 0))


def solution(mesh):
    return jax.shard_map(
        on_device,
        mesh=mesh,
        in_specs=(
            P("rows", None, None),
            P("rows"),
            P("rows"),
            P("rows"),
            P("rows", None, None),
            P("rows", None, None),
        ),
        out_specs=(P("rows", None, None), P()),
        check_vma=False,
    )
```
